32 devices in a mesh: dev: 8 (over z, y), rep: 4 (over x, core).
Axes of the slice: x: 2, y: 2, z: 4, core: 2. Of those that a mesh axis runs over, the one named last changes fastest.
Arguments:
- features: bfloat16 [32768, 256], P(('dev', 'rep')), may hold values from -6 to 6
- history: bfloat16 [32768, 256], P(('dev', 'rep')), may hold values from -6 to 6
- new_owner: int32 [32, 8], P(('dev', 'rep')), may hold values from 0 to 7, as said below
- pull_rows: int32 [32768], P(('dev', 'rep')), may hold values from 0 to 1023
- occupancy: int32 [256, 16], P(('dev', 'rep')), may hold values from 0 to 1, as said below
- adj_local: bfloat16 [32768, 1024], P(('dev', 'rep')), may hold values from -0.125 to 0.125
- adj_boundary: bfloat16 [32768, 1024], P(('dev', 'rep')), may hold values from -0.125 to 0.125
- w_first: bfloat16 [256, 256], replicated, may hold values from -0.375 to 0.375
- bias_first: float32 [256], replicated, may hold values from -3 to 3
- w_second: bfloat16 [256, 256], replicated, may hold values from -0.375 to 0.375
- cotangent: bfloat16 [32768, 256], P(('dev', 'rep')), may hold values from -6 to 6
Outputs:
- hidden: bfloat16 [32768, 256], P(('dev', 'rep'))
- output: bfloat16 [32768, 256], P(('dev', 'rep'))
- w_second_grad: float32 [256, 256], replicated
The draws below stay inside these ranges and needn't reach their ends.
Inputs may be any that keep to these rules, and one draw needn't show every extreme that they name: Each row of new_owner is a permutation of 0 to 7. `occupancy`: tile flags of 0 or 1.
All inputs are finite; a program needn't handle non-finite values.
Results may differ from the reference program's by a relative error of at most 0.0061.
Values may be sent and summed in bfloat16 or wider, within the bound.
A program may use at most 64 MiB of HBM per device.

```python
import jax
import jax.numpy as jnp
from jax import lax

F = 256
ROWS_DEV = 1024
PULL_DEV = 1024
NODES = 32768
N_DEV = 8
N_REP = 4


def draw_new_owner(key, part):
    keys = jax.random.split(jax.random.fold_in(key, 11), N_DEV * N_REP)

    def shuffle(single):
        return jax.random.permutation(single, N_DEV)
    return jax.vmap(shuffle)(keys).astype(jnp.int32)


def draw_occupancy(key, part):
    tile_rows = ROWS_DEV // 128
    tile_cols = (ROWS_DEV + PULL_DEV) // 128
    total = N_DEV * N_REP
    first, second = jax.random.split(jax.random.fold_in(key, 23))
    level = jax.random.randint(first, (total, 1, 1), 1, 5)
    rolled = jax.random.randint(second, (total, tile_rows, tile_cols), 0, 4)
    return (rolled < level).astype(jnp.int32).reshape(total * tile_rows, tile_cols)


def set_ends(entries, stream_key, smallest, top_value):
    spot = [jax.random.randint(jax.random.fold_in(stream_key, axis), (), 0, length) for axis, length in enumerate(entries.shape)]
    longest = entries.shape.index(max(entries.shape))
    next_to = spot[:longest] + [(spot[longest] + 1) % entries.shape[longest]] + spot[longest + 1:]
    return entries.at[tuple(spot)].set(smallest).at[tuple(next_to)].set(top_value)


def with_spikes(values, rng, source, target, shards_of, factor):
    def block_of(dim):
        return (jnp.arange(values.shape[dim]) // (values.shape[dim] // shards_of)).reshape((-1,) + (1,) * (values.ndim - 1 - dim))

    first = jax.random.permutation(rng, shards_of)[block_of(target)]
    other_side = (block_of(target) + shards_of // 2) % shards_of
    return jnp.where((block_of(source) == first) | (block_of(source) == other_side), factor * values, values)


def block_scale(stream_key, dims, shards, low, high):
    def one(dim, shards_of):
        draws = jax.random.uniform(jax.random.fold_in(jax.random.fold_in(stream_key, 6), dim), (shards_of,), jnp.float32, low / len(shards), high / len(shards))
        return jnp.repeat(jnp.exp(draws), dims[dim] // shards_of).reshape((-1,) + (1,) * (len(dims) - dim - 1))

    loudness = one(*shards[0])
    for cut in shards[1:]:
        loudness = loudness * one(*cut)
    return loudness


def bell_draw(stream_key, dims, scale, limit, cuts=(), kind=jnp.bfloat16):
    loudness = block_scale(stream_key, dims, cuts, -0.22, 0.18) if cuts else 1.0
    values = jax.random.normal(stream_key, dims, jnp.float32) * scale * loudness
    return jnp.minimum(jnp.maximum(values, -limit), limit).astype(kind)


def gaussian_with(stream_key, extent, scale, bound, cuts, heavy, kind=jnp.bfloat16):
    array = scale * jax.random.normal(stream_key, extent, jnp.float32)
    if cuts:
        array = array * block_scale(stream_key, extent, cuts, -0.22, 0.18)
    return jnp.clip(with_spikes(array, jax.random.fold_in(stream_key, 3), *heavy), -bound, bound).astype(kind)


def setup_inputs(seed: int = 0) -> dict:
    splits = jax.random.split(jax.random.key(seed), 12)
    features = bell_draw(splits[0], (NODES, F), 1.0, 6.0, ((0, 32),))
    history = bell_draw(splits[1], (NODES, F), 1.0, 6.0, ((0, 32),))
    new_owner = draw_new_owner(jax.random.fold_in(splits[11], 71), 0)
    pull_rows = set_ends(jax.random.randint(splits[3], (N_DEV * N_REP * PULL_DEV,), 0, ROWS_DEV), jax.random.fold_in(splits[3], 1), 0, ROWS_DEV - 1).astype(jnp.int32)
    occupancy = draw_occupancy(jax.random.fold_in(splits[11], 71), 0)
    adj_local = bell_draw(splits[5], (NODES, ROWS_DEV), (ROWS_DEV + PULL_DEV) ** -0.5, 0.125, ((0, 32),))
    adj_boundary = bell_draw(splits[6], (NODES, PULL_DEV), (ROWS_DEV + PULL_DEV) ** -0.5, 0.125, ((0, 32),))
    w_first = bell_draw(splits[7], (F, F), F ** -0.5, 0.375)
    bias_first = bell_draw(splits[8], (F,), 0.5, 3.0, (), jnp.float32)
    w_second = bell_draw(splits[9], (F, F), F ** -0.5, 0.375)
    cotangent = gaussian_with(splits[10], (NODES, F), 1.0, 6.0, ((0, 32),), (0, 1, 32, 2.75))
    return dict(features=features, history=history, new_owner=new_owner, pull_rows=pull_rows, occupancy=occupancy, adj_local=adj_local, adj_boundary=adj_boundary, w_first=w_first, bias_first=bias_first, w_second=w_second, cotangent=cotangent)


def expand(occupied):
    return jnp.repeat(jnp.repeat(occupied, 128, axis=-2), 128, axis=-1).astype(jnp.bfloat16)


def reference(features, history, new_owner, pull_rows, occupancy, adj_local, adj_boundary, w_first, bias_first, w_second, cotangent):
    peer_count = N_DEV
    copies = N_REP
    height = ROWS_DEV
    breadth = F
    cluster = height // peer_count
    pulled = PULL_DEV
    per_peer = pulled // peer_count
    indices = jnp.arange(peer_count, dtype=jnp.int32)
    routes = new_owner.reshape(peer_count, copies, peer_count)
    matches = (routes[:, :, :, None] == indices).astype(jnp.int32)
    inverse = jnp.sum(matches * indices[:, None], axis=2).astype(jnp.int32)

    def migrate(values):
        blocks = values.reshape(peer_count, copies, peer_count, cluster, breadth)
        where_from = jnp.broadcast_to(inverse[:, :, :, None, None], blocks.shape)
        arrived = jnp.take_along_axis(blocks, where_from, axis=2)
        return arrived.transpose(2, 1, 0, 3, 4).reshape(peer_count, copies, height, breadth)

    own_x = migrate(features)
    own_h = migrate(history)
    wanted = pull_rows.reshape(peer_count, copies, pulled)
    owners = jnp.arange(pulled, dtype=jnp.int32) // per_peer
    flat_rows = (owners[None, None, :] * height + wanted).astype(jnp.int32)
    replica_ids = jnp.arange(copies, dtype=jnp.int32)[None, :, None]

    def fetch_remote(values):
        spread = values.transpose(1, 0, 2, 3).reshape(copies, peer_count * height, breadth)
        return spread[replica_ids, flat_rows]

    def scatter(partial_value):
        summed = jnp.zeros((copies, peer_count * height, breadth), jnp.float32)
        summed = summed.at[replica_ids, flat_rows].add(partial_value.astype(jnp.float32))
        summed = summed.reshape(copies, peer_count, height, breadth).transpose(1, 0, 2, 3)
        return summed.reshape(peer_count * copies * height, breadth)

    tile_mask = occupancy.reshape(peer_count * copies, height // 128, (height + pulled) // 128)
    local_adj = adj_local.reshape(peer_count * copies, height, height)
    edge_adj = adj_boundary.reshape(peer_count * copies, height, pulled)

    def layer_terms(owned, remote):
        def device(operands):
            owned_rows, theirs, local_tile, edge_tile, flags = operands
            full_mask = expand(flags)
            local_tile = local_tile * full_mask[:, :height]
            edge_tile = edge_tile * full_mask[:, height:]
            summed = jnp.dot(local_tile, owned_rows, preferred_element_type=jnp.float32)
            summed = summed + jnp.dot(edge_tile, theirs, preferred_element_type=jnp.float32)
            partial_value = lax.dot_general(edge_tile, owned_rows, (((0,), (0,)), ((), ())), preferred_element_type=jnp.float32)
            return summed, partial_value.astype(jnp.bfloat16)

        summed, partial_value = lax.map(device, (owned.reshape(-1, height, breadth), remote.reshape(-1, pulled, breadth), local_adj, edge_adj, tile_mask))
        return summed.reshape(-1, breadth), partial_value.reshape(peer_count, copies, pulled, breadth)

    summed_one, partial_one = layer_terms(own_x, fetch_remote(own_x))
    aggregate_one = (summed_one + scatter(partial_one)).astype(jnp.bfloat16)
    hidden = jnp.maximum(jnp.dot(aggregate_one, w_first, preferred_element_type=jnp.float32) + bias_first, 0.0).astype(jnp.bfloat16)
    summed_two, partial_two = layer_terms(hidden.reshape(peer_count, copies, height, breadth), fetch_remote(own_h))
    aggregate_two = (summed_two + scatter(partial_two)).astype(jnp.bfloat16)
    output = jnp.dot(aggregate_two, w_second, preferred_element_type=jnp.float32).astype(jnp.bfloat16)
    gradient = lax.dot_general(aggregate_two, cotangent, (((0,), (0,)), ((), ())), preferred_element_type=jnp.float32)
    return hidden, output, gradient
```

```python
import functools

import jax
import jax.numpy as jnp
from jax import lax
from jax.experimental import pallas as pl
from jax.experimental.pallas import tpu as pltpu
from jax.sharding import PartitionSpec as P

MESH = pl.DeviceIdType.MESH
F32 = jnp.float32
BF16 = jnp.bfloat16
ASK, MOVE_X, MOVE_H, FAR_X, FAR_H, PUSH_ONE, PUSH_TWO, SCATTER, GATHER = range(9)


def step_kernel(
    n,
    reps,
    features,
    history,
    new_owner,
    pulls,
    occupancy,
    adj_local_hbm,
    adj_edge_hbm,
    w_first,
    bias_first,
    w_second,
    cotangent_hbm,
    hidden_out,
    output_out,
    grad_out,
    local,
    edge,
    edge_t,
    cotangent,
    asked,
    pick,
    pick_t,
    send_x,
    send_h,
    own_x,
    own_h,
    send_far_x,
    send_far_h,
    far_x,
    far_h,
    send_one,
    send_two,
    push_one,
    push_two,
    acc,
    hidden,
    agg,
    grad_mine,
    grad_rep,
    sum_rep,
    grad_dev,
    sum_dev,
    grad_rows,
    grad_all,
    load_sem,
    send_sem,
    recv_sem,
    rep_send,
    rep_recv,
):
    me = lax.axis_index("dev")
    my_rep = lax.axis_index("rep")
    height, breadth = features.shape
    cluster = height // n
    per_peer = pulls.shape[2]
    pulled = n * per_peer
    tile = height // occupancy.shape[0]
    band = min(256, height)

    def peer(off):
        return lax.rem(me + off, n)

    def rep_peer(off):
        return lax.rem(my_rep + off, reps)

    loads = [
        pltpu.make_async_copy(adj_edge_hbm, edge, load_sem.at[0]),
        pltpu.make_async_copy(adj_local_hbm, local, load_sem.at[1]),
        pltpu.make_async_copy(cotangent_hbm, cotangent, load_sem.at[2]),
    ]
    for load in loads:
        load.start()

    barrier = pltpu.get_barrier_semaphore()
    for off in range(1, n):
        pl.semaphore_signal(barrier, inc=1, device_id={"dev": peer(off)}, device_id_type=MESH)
    for off in range(1, reps):
        pl.semaphore_signal(barrier, inc=1, device_id={"rep": rep_peer(off)}, device_id_type=MESH)

    def cluster_for(source, owner):
        block = jnp.zeros((cluster, breadth), BF16)
        for j in range(n):
            chosen = jnp.where(new_owner[0, j] == owner, 1.0, 0.0)
            weight = jnp.full((cluster, breadth), chosen, F32).astype(BF16)
            block = block + source[j * cluster : (j + 1) * cluster, :] * weight
        return block

    def outgoing(phase, src, dst, to, slot):
        return pltpu.make_async_remote_copy(
            src_ref=src.at[to],
            dst_ref=dst.at[slot],
            send_sem=send_sem.at[phase, to],
            recv_sem=recv_sem.at[phase, slot],
            device_id={"dev": to},
            device_id_type=MESH,
        )

    def send(phase, src, dst, off):
        outgoing(phase, src, dst, peer(off), me).start()

    def receive(phase, src, dst):
        for off in range(1, n):
            other = peer(off)
            outgoing(phase, src, dst, other, other).wait_recv()

    def finish(phase, src, dst):
        for off in range(1, n):
            outgoing(phase, src, dst, peer(off), me).wait_send()

    for off in range(1, n):
        send_x[peer(off)] = cluster_for(features, peer(off))
    own_x[me] = cluster_for(features, me)
    pl.semaphore_wait(barrier, n - 1 + reps - 1)
    for off in range(1, n):
        send(ASK, pulls, asked, off)
    for off in range(1, n):
        send(MOVE_X, send_x, own_x, off)
    for off in range(1, n):
        send_h[peer(off)] = cluster_for(history, peer(off))
        send(MOVE_H, send_h, own_h, off)
    own_h[me] = cluster_for(history, me)
    asked[me] = pulls[me]

    loads[0].wait()
    for i in range(height // tile):
        for j in range(pulled // tile):
            kept = occupancy[i, height // tile + j].astype(F32)
            rows, cols = pl.ds(i * tile, tile), pl.ds(j * tile, tile)
            part = (edge[rows, cols].astype(F32) * kept).astype(BF16)
            edge[rows, cols] = part
            edge_t[cols, rows] = part.T
    loads[1].wait()
    for i in range(height // tile):
        for j in range(height // tile):
            kept = occupancy[i, j].astype(F32)
            rows, cols = pl.ds(i * tile, tile), pl.ds(j * tile, tile)
            local[rows, cols] = (local[rows, cols].astype(F32) * kept).astype(BF16)

    receive(ASK, pulls, asked)
    for d in range(n):
        wanted = asked[d]
        rows = lax.broadcasted_iota(jnp.int32, (height, per_peer), 0)
        pick[:, d * per_peer : (d + 1) * per_peer] = jnp.where(rows == wanted, 1.0, 0.0).astype(
            BF16
        )
        turned = jnp.broadcast_to(wanted, (per_peer, per_peer)).T
        lanes = lax.broadcasted_iota(jnp.int32, (per_peer, per_peer), 1)
        for c in range(height // per_peer):
            pick_t[d * per_peer : (d + 1) * per_peer, c * per_peer : (c + 1) * per_peer] = (
                jnp.where(turned == lanes + c * per_peer, 1.0, 0.0).astype(BF16)
            )

    def blocks_out(phase, left, right, src, dst):
        values = right[...].reshape(left.shape[1], breadth)

        def block(to):
            rows = pl.ds(pl.multiple_of(to * per_peer, per_peer), per_peer)
            return jnp.dot(left[rows, :], values, preferred_element_type=F32).astype(BF16)

        def one(off, carry):
            src[peer(off)] = block(peer(off))
            send(phase, src, dst, off)
            return carry

        lax.fori_loop(1, n, one, 0)
        dst[me] = block(me)

    def bands(body):
        def one(i, carry):
            body(pl.ds(pl.multiple_of(i * band, band), band))
            return carry

        lax.fori_loop(0, height // band, one, 0)

    def times(left, rows, right):
        values = right[...].reshape(left.shape[1], breadth)
        return jnp.dot(left[rows, :], values, preferred_element_type=F32)

    receive(MOVE_X, send_x, own_x)
    blocks_out(FAR_X, pick_t, own_x, send_far_x, far_x)
    blocks_out(PUSH_ONE, edge_t, own_x, send_one, push_one)

    def local_one(rows):
        acc[rows, :] = times(local, rows, own_x)

    bands(local_one)
    receive(MOVE_H, send_h, own_h)
    blocks_out(FAR_H, pick_t, own_h, send_far_h, far_h)
    receive(FAR_X, send_far_x, far_x)

    def edge_one(rows):
        acc[rows, :] = acc[rows, :] + times(edge, rows, far_x)

    bands(edge_one)
    receive(PUSH_ONE, send_one, push_one)

    def first(rows):
        total = (acc[rows, :] + times(pick, rows, push_one)).astype(BF16)
        value = jnp.dot(total, w_first[...], preferred_element_type=F32) + bias_first[...]
        value = jnp.maximum(value, 0.0).astype(BF16)
        hidden[rows, :] = value
        hidden_out[rows, :] = value

    bands(first)
    blocks_out(PUSH_TWO, edge_t, hidden, send_two, push_two)

    def local_two(rows):
        acc[rows, :] = times(local, rows, hidden)

    bands(local_two)
    receive(FAR_H, send_far_h, far_h)

    def edge_two(rows):
        acc[rows, :] = acc[rows, :] + times(edge, rows, far_h)

    bands(edge_two)
    loads[2].wait()
    receive(PUSH_TWO, send_two, push_two)

    def second(rows):
        agg[rows, :] = (acc[rows, :] + times(pick, rows, push_two)).astype(BF16)

    bands(second)
    grad = lax.dot_general(
        agg[...], cotangent[...], (((0,), (0,)), ((), ())), preferred_element_type=F32
    )
    grad_mine[...] = grad.reshape(grad_mine.shape)

    def across(phase, src, dst, to, slot):
        return pltpu.make_async_remote_copy(
            src_ref=src,
            dst_ref=dst.at[slot],
            send_sem=rep_send.at[phase, to],
            recv_sem=rep_recv.at[phase, slot],
            device_id={"rep": to},
            device_id_type=MESH,
        )

    def share(src, dst, to, slot):
        return pltpu.make_async_remote_copy(
            src_ref=src,
            dst_ref=dst.at[slot],
            send_sem=send_sem.at[GATHER, to],
            recv_sem=recv_sem.at[GATHER, slot],
            device_id={"dev": to},
            device_id_type=MESH,
        )

    for off in range(1, reps):
        to = rep_peer(off)
        across(0, grad_mine.at[to], grad_rep, to, my_rep).start()

    def last(rows):
        output_out[rows, :] = jnp.dot(
            agg[rows, :], w_second[...], preferred_element_type=F32
        ).astype(BF16)

    bands(last)
    total = grad_mine[my_rep]
    for off in range(1, reps):
        to = rep_peer(off)
        across(0, grad_mine.at[to], grad_rep, to, to).wait_recv()
        total = total + grad_rep[to]
    sum_rep[...] = total
    for off in range(1, n):
        send(SCATTER, sum_rep, grad_dev, off)
    receive(SCATTER, sum_rep, grad_dev)
    grad_dev[me] = sum_rep[me]
    rows_sum = grad_dev[0]
    for d in range(1, n):
        rows_sum = rows_sum + grad_dev[d]
    sum_dev[...] = rows_sum
    for off in range(1, n):
        share(sum_dev, grad_rows, peer(off), me).start()
    grad_rows[me] = rows_sum
    for off in range(1, n):
        share(sum_dev, grad_rows, peer(off), peer(off)).wait_recv()
    for off in range(1, reps):
        across(1, grad_rows, grad_all, rep_peer(off), my_rep).start()
    grad_all[my_rep] = grad_rows[...]
    for off in range(1, reps):
        across(1, grad_rows, grad_all, rep_peer(off), rep_peer(off)).wait_recv()
    grad_out[...] = grad_all[...]

    finish(ASK, pulls, asked)
    finish(MOVE_X, send_x, own_x)
    finish(MOVE_H, send_h, own_h)
    finish(FAR_X, send_far_x, far_x)
    finish(FAR_H, send_far_h, far_h)
    finish(PUSH_ONE, send_one, push_one)
    finish(PUSH_TWO, send_two, push_two)
    finish(SCATTER, sum_rep, grad_dev)
    for off in range(1, n):
        share(sum_dev, grad_rows, peer(off), me).wait_send()
    for off in range(1, reps):
        to = rep_peer(off)
        across(0, grad_mine.at[to], grad_rep, to, my_rep).wait_send()
        across(1, grad_rows, grad_all, to, my_rep).wait_send()


def fused(
    features,
    history,
    new_owner,
    pull_rows,
    occupancy,
    adj_local,
    adj_boundary,
    w_first,
    bias_first,
    w_second,
    cotangent,
):
    n, reps = lax.axis_size("dev"), lax.axis_size("rep")
    height, breadth = features.shape
    cluster = height // n
    pulled = pull_rows.shape[0]
    per_peer = pulled // n
    part = breadth // (n * reps)
    vmem = pl.BlockSpec(memory_space=pltpu.VMEM)
    smem = pl.BlockSpec(memory_space=pltpu.SMEM)
    anywhere = pl.BlockSpec(memory_space=pl.ANY)
    moved = pltpu.VMEM((n, cluster, breadth), BF16)
    listed = pltpu.VMEM((n, per_peer, breadth), BF16)
    strip = pltpu.VMEM((n, part, breadth), F32)
    square = pltpu.VMEM((reps, n, part, breadth), F32)
    hidden, output, gradient = pl.pallas_call(
        functools.partial(step_kernel, n, reps),
        out_shape=(
            jax.ShapeDtypeStruct((height, breadth), BF16),
            jax.ShapeDtypeStruct((height, breadth), BF16),
            jax.ShapeDtypeStruct((reps, n, part, breadth), F32),
        ),
        in_specs=[
            vmem,
            vmem,
            smem,
            vmem,
            smem,
            anywhere,
            anywhere,
            vmem,
            vmem,
            vmem,
            anywhere,
        ],
        out_specs=(vmem, vmem, vmem),
        scratch_shapes=[
            pltpu.VMEM((height, height), BF16),
            pltpu.VMEM((height, pulled), BF16),
            pltpu.VMEM((pulled, height), BF16),
            pltpu.VMEM((height, breadth), BF16),
            pltpu.VMEM((n, 1, per_peer), jnp.int32),
            pltpu.VMEM((height, pulled), BF16),
            pltpu.VMEM((pulled, height), BF16),
            moved,
            moved,
            moved,
            moved,
            listed,
            listed,
            listed,
            listed,
            listed,
            listed,
            listed,
            listed,
            pltpu.VMEM((height, breadth), F32),
            pltpu.VMEM((height, breadth), BF16),
            pltpu.VMEM((height, breadth), BF16),
            square,
            square,
            strip,
            strip,
            pltpu.VMEM((part, breadth), F32),
            strip,
            square,
            pltpu.SemaphoreType.DMA((3,)),
            pltpu.SemaphoreType.DMA((9, n)),
            pltpu.SemaphoreType.DMA((9, n)),
            pltpu.SemaphoreType.DMA((2, reps)),
            pltpu.SemaphoreType.DMA((2, reps)),
        ],
        compiler_params=pltpu.CompilerParams(
            collective_id=0, has_side_effects=True, vmem_limit_bytes=56 * 1024 * 1024
        ),
    )(
        features,
        history,
        new_owner,
        pull_rows.reshape(n, 1, per_peer),
        occupancy,
        adj_local,
        adj_boundary,
        w_first,
        bias_first.reshape(1, breadth),
        w_second,
        cotangent,
    )
    return hidden, output, gradient.reshape(breadth, breadth)


def fits(peers, height, pulled, breadth, everyone):
    return (
        height % (128 * peers) == 0 and pulled == 128 * peers and breadth % (8 * everyone) == 0
    )


def expand(occupied):
    return jnp.repeat(jnp.repeat(occupied, 128, axis=0), 128, axis=1).astype(jnp.bfloat16)


def dense_terms(owned, remote, adj_local, adj_boundary, occupancy):
    height = owned.shape[0]
    full_mask = expand(occupancy)
    local_tile = adj_local * full_mask[:, :height]
    edge_tile = adj_boundary * full_mask[:, height:]
    summed = jnp.dot(local_tile, owned, preferred_element_type=jnp.float32)
    summed = summed + jnp.dot(edge_tile, remote, preferred_element_type=jnp.float32)
    partial_value = lax.dot_general(
        edge_tile, owned, (((0,), (0,)), ((), ())), preferred_element_type=jnp.float32
    )
    return (summed, partial_value)


def body(
    features,
    history,
    new_owner,
    pull_rows,
    occupancy,
    adj_local,
    adj_boundary,
    w_first,
    bias_first,
    w_second,
    cotangent,
):
    peer_count = lax.axis_size("dev")
    height, breadth = features.shape
    cluster = height // peer_count
    pulled = pull_rows.shape[0]
    per_peer = pulled // peer_count
    everyone = peer_count * lax.axis_size("rep")
    if fits(peer_count, height, pulled, breadth, everyone):
        return fused(
            features,
            history,
            new_owner,
            pull_rows,
            occupancy,
            adj_local,
            adj_boundary,
            w_first,
            bias_first,
            w_second,
            cotangent,
        )
    indices = jnp.arange(peer_count, dtype=jnp.int32)
    matches = (new_owner[0][:, None] == indices[None, :]).astype(jnp.int32)
    inverse = jnp.sum(matches * indices[:, None], axis=0)

    def arrange(values):
        return values.reshape(peer_count, cluster, breadth)[inverse]

    requests = lax.all_to_all(
        pull_rows.reshape(peer_count, per_peer), "dev", split_axis=0, concat_axis=0, tiled=True
    ).reshape(pulled)

    def fetch_rows(values):
        return values[requests].reshape(peer_count, per_peer, breadth)

    selector = (requests[None, :] == jnp.arange(height, dtype=jnp.int32)[:, None]).astype(
        jnp.bfloat16
    )

    def collect(received):
        return jnp.dot(
            selector, received.reshape(pulled, breadth), preferred_element_type=jnp.float32
        )

    def layer_terms(owned, remote):
        return dense_terms(owned, remote, adj_local, adj_boundary, occupancy)

    moved_x, moved_h = (
        lax.all_to_all(arrange(features), "dev", split_axis=0, concat_axis=0, tiled=True),
        lax.all_to_all(arrange(history), "dev", split_axis=0, concat_axis=0, tiled=True),
    )
    own_x = moved_x.reshape(height, breadth)
    own_h = moved_h.reshape(height, breadth)
    far_x, far_h = (
        lax.all_to_all(fetch_rows(own_x), "dev", split_axis=0, concat_axis=0, tiled=True),
        lax.all_to_all(fetch_rows(own_h), "dev", split_axis=0, concat_axis=0, tiled=True),
    )
    summed_one, partial_one = layer_terms(own_x, far_x.reshape(pulled, breadth))
    pushed_one = lax.all_to_all(
        partial_one.astype(jnp.bfloat16).reshape(peer_count, per_peer, breadth),
        "dev",
        split_axis=0,
        concat_axis=0,
        tiled=True,
    )
    far_h = far_h.reshape(pulled, breadth)
    aggregate_one = (summed_one + collect(pushed_one)).astype(jnp.bfloat16)
    hidden = jnp.maximum(
        jnp.dot(aggregate_one, w_first, preferred_element_type=jnp.float32) + bias_first, 0.0
    ).astype(jnp.bfloat16)
    summed_two, partial_two = layer_terms(hidden, far_h)
    pushed_two = lax.all_to_all(
        partial_two.astype(jnp.bfloat16).reshape(peer_count, per_peer, breadth),
        "dev",
        split_axis=0,
        concat_axis=0,
        tiled=True,
    )
    aggregate_two = (summed_two + collect(pushed_two)).astype(jnp.bfloat16)
    output = jnp.dot(aggregate_two, w_second, preferred_element_type=jnp.float32).astype(
        jnp.bfloat16
    )
    local_grad = lax.dot_general(
        aggregate_two, cotangent, (((0,), (0,)), ((), ())), preferred_element_type=jnp.float32
    )
    slices = lax.all_to_all(
        local_grad.reshape(everyone, breadth // everyone, breadth),
        ("dev", "rep"),
        split_axis=0,
        concat_axis=0,
        tiled=True,
    )
    gradient = lax.all_gather(jnp.sum(slices, axis=0), ("dev", "rep"), axis=0, tiled=True)
    return (hidden, output, gradient)


def solution(mesh):
    return jax.shard_map(
        body,
        mesh=mesh,
        in_specs=(
            P(("dev", "rep"), None),
            P(("dev", "rep"), None),
            P(("dev", "rep"), None),
            P(("dev", "rep")),
            P(("dev", "rep"), None),
            P(("dev", "rep"), None),
            P(("dev", "rep"), None),
            P(),
            P(),
            P(),
            P(("dev", "rep"), None),
        ),
        out_specs=(P(("dev", "rep"), None), P(("dev", "rep"), None), P()),
        check_vma=False,
    )
```

```python
import functools

import jax
import jax.numpy as jnp
from jax import lax
from jax.experimental import pallas as pl
from jax.experimental.pallas import tpu as pltpu
from jax.sharding import PartitionSpec as P

MESH = pl.DeviceIdType.MESH
F32 = jnp.float32
BF16 = jnp.bfloat16
ASK, MOVE_X, MOVE_H, FAR_X, FAR_H, PUSH_ONE, PUSH_TWO, SCATTER, GATHER = range(9)


def step_kernel(
    n,
    reps,
    features,
    history_hbm,
    new_owner,
    pulls,
    occupancy,
    adj_local_hbm,
    adj_edge_hbm,
    w_first,
    bias_first,
    cotangent_hbm,
    pre_out,
    agg_out,
    grad_out,
    history,
    local,
    edge,
    edge_t,
    cotangent,
    asked,
    pick,
    pick_t,
    send_x,
    send_h,
    own_x,
    own_h,
    send_far_x,
    send_far_h,
    far_x,
    far_h,
    send_one,
    send_two,
    push_one,
    push_two,
    acc,
    pre,
    hidden,
    agg,
    grad_mine,
    grad_rep,
    sum_rep,
    grad_dev,
    sum_dev,
    grad_rows,
    grad_all,
    load_sem,
    send_sem,
    recv_sem,
    rep_send,
    rep_recv,
):
    me = lax.axis_index("dev")
    my_rep = lax.axis_index("rep")
    height, breadth = features.shape
    cluster = height // n
    per_peer = pulls.shape[2]
    pulled = n * per_peer
    tile = height // occupancy.shape[0]
    band = min(256, height)

    side = 1 - 2 * (me // (n // 2))

    def peer(off):
        return lax.rem(me + side * off + n, n)

    def rep_peer(off):
        return lax.rem(my_rep + off, reps)

    loads = [
        pltpu.make_async_copy(adj_edge_hbm, edge, load_sem.at[0]),
        pltpu.make_async_copy(adj_local_hbm, local, load_sem.at[1]),
        pltpu.make_async_copy(cotangent_hbm, cotangent, load_sem.at[2]),
        pltpu.make_async_copy(history_hbm, history, load_sem.at[3]),
    ]
    for k in (3, 0, 1, 2):
        loads[k].start()

    barrier = pltpu.get_barrier_semaphore()
    for off in range(1, n):
        pl.semaphore_signal(barrier, inc=1, device_id={"dev": peer(off)}, device_id_type=MESH)
    for off in range(1, reps):
        pl.semaphore_signal(barrier, inc=1, device_id={"rep": rep_peer(off)}, device_id_type=MESH)

    def cluster_for(source, owner):
        block = jnp.zeros((cluster, breadth), BF16)
        for j in range(n):
            chosen = jnp.where(new_owner[0, j] == owner, 1.0, 0.0)
            weight = jnp.full((cluster, breadth), chosen, F32).astype(BF16)
            block = block + source[j * cluster : (j + 1) * cluster, :] * weight
        return block

    def outgoing(phase, src, dst, to, slot):
        return pltpu.make_async_remote_copy(
            src_ref=src.at[to],
            dst_ref=dst.at[slot],
            send_sem=send_sem.at[phase, to],
            recv_sem=recv_sem.at[phase, slot],
            device_id={"dev": to},
            device_id_type=MESH,
        )

    def send(phase, src, dst, off):
        outgoing(phase, src, dst, peer(off), me).start()

    def receive(phase, src, dst):
        for off in range(1, n):
            other = peer(off)
            outgoing(phase, src, dst, other, other).wait_recv()

    def finish(phase, src, dst):
        for off in range(1, n):
            outgoing(phase, src, dst, peer(off), me).wait_send()

    for off in range(1, n):
        send_x[peer(off)] = cluster_for(features, peer(off))
    own_x[me] = cluster_for(features, me)
    pl.semaphore_wait(barrier, n - 1 + reps - 1)
    for off in range(1, n):
        send(ASK, pulls, asked, off)
    for off in range(1, n):
        send(MOVE_X, send_x, own_x, off)
    loads[3].wait()
    for off in range(1, n):
        send_h[peer(off)] = cluster_for(history, peer(off))
        send(MOVE_H, send_h, own_h, off)
    own_h[me] = cluster_for(history, me)
    asked[me] = pulls[me]

    loads[0].wait()
    for i in range(height // tile):
        for j in range(pulled // tile):
            kept = occupancy[i, height // tile + j].astype(F32)
            rows, cols = pl.ds(i * tile, tile), pl.ds(j * tile, tile)
            part = (edge[rows, cols].astype(F32) * kept).astype(BF16)
            edge[rows, cols] = part
            edge_t[cols, rows] = part.T
    loads[1].wait()
    for i in range(height // tile):
        for j in range(height // tile):
            kept = occupancy[i, j].astype(F32)
            rows, cols = pl.ds(i * tile, tile), pl.ds(j * tile, tile)
            local[rows, cols] = (local[rows, cols].astype(F32) * kept).astype(BF16)

    receive(ASK, pulls, asked)
    for d in range(n):
        wanted = asked[d]
        rows = lax.broadcasted_iota(jnp.int32, (height, per_peer), 0)
        pick[:, d * per_peer : (d + 1) * per_peer] = jnp.where(rows == wanted, 1.0, 0.0).astype(
            BF16
        )
        turned = jnp.broadcast_to(wanted, (per_peer, per_peer)).T
        lanes = lax.broadcasted_iota(jnp.int32, (per_peer, per_peer), 1)
        for c in range(height // per_peer):
            pick_t[d * per_peer : (d + 1) * per_peer, c * per_peer : (c + 1) * per_peer] = (
                jnp.where(turned == lanes + c * per_peer, 1.0, 0.0).astype(BF16)
            )

    def blocks_out(phase, left, right, src, dst):
        values = right[...].reshape(left.shape[1], breadth)

        def block(to):
            rows = pl.ds(pl.multiple_of(to * per_peer, per_peer), per_peer)
            return jnp.dot(left[rows, :], values, preferred_element_type=F32).astype(BF16)

        def one(off, carry):
            src[peer(off)] = block(peer(off))
            send(phase, src, dst, off)
            return carry

        lax.fori_loop(1, n, one, 0)
        dst[me] = block(me)

    def bands(body):
        def one(i, carry):
            body(pl.ds(pl.multiple_of(i * band, band), band))
            return carry

        lax.fori_loop(0, height // band, one, 0)

    def times(left, rows, right):
        values = right[...].reshape(left.shape[1], breadth)
        return jnp.dot(left[rows, :], values, preferred_element_type=F32)

    receive(MOVE_X, send_x, own_x)
    blocks_out(FAR_X, pick_t, own_x, send_far_x, far_x)
    blocks_out(PUSH_ONE, edge_t, own_x, send_one, push_one)

    def local_one(rows):
        acc[rows, :] = times(local, rows, own_x)

    bands(local_one)
    receive(MOVE_H, send_h, own_h)
    blocks_out(FAR_H, pick_t, own_h, send_far_h, far_h)
    receive(FAR_X, send_far_x, far_x)

    def edge_one(rows):
        acc[rows, :] = acc[rows, :] + times(edge, rows, far_x)

    bands(edge_one)
    receive(PUSH_ONE, send_one, push_one)

    def first(rows):
        total = (acc[rows, :] + times(pick, rows, push_one)).astype(BF16)
        value = jnp.dot(total, w_first[...], preferred_element_type=F32) + bias_first[...]
        pre[rows, :] = value.astype(BF16)
        hidden[rows, :] = jnp.maximum(value, 0.0).astype(BF16)

    bands(first)
    blocks_out(PUSH_TWO, edge_t, hidden, send_two, push_two)
    store_pre = pltpu.make_async_copy(pre, pre_out, load_sem.at[0])
    store_pre.start()

    def local_two(rows):
        acc[rows, :] = times(local, rows, hidden)

    bands(local_two)
    receive(FAR_H, send_far_h, far_h)

    def edge_two(rows):
        acc[rows, :] = acc[rows, :] + times(edge, rows, far_h)

    bands(edge_two)
    loads[2].wait()
    receive(PUSH_TWO, send_two, push_two)

    def second(rows):
        agg[rows, :] = (acc[rows, :] + times(pick, rows, push_two)).astype(BF16)

    bands(second)
    store_agg = pltpu.make_async_copy(agg, agg_out, load_sem.at[1])
    grad = lax.dot_general(
        agg[...], cotangent[...], (((0,), (0,)), ((), ())), preferred_element_type=F32
    )
    grad_mine[...] = grad.reshape(grad_mine.shape)

    def across(phase, src, dst, to, slot, piece):
        return pltpu.make_async_remote_copy(
            src_ref=src,
            dst_ref=dst.at[slot, piece],
            send_sem=rep_send.at[phase, to, piece],
            recv_sem=rep_recv.at[phase, slot, piece],
            device_id={"rep": to},
            device_id_type=MESH,
        )

    def share(src, dst, to, slot):
        return pltpu.make_async_remote_copy(
            src_ref=src,
            dst_ref=dst.at[slot],
            send_sem=send_sem.at[GATHER, to],
            recv_sem=recv_sem.at[GATHER, slot],
            device_id={"dev": to},
            device_id_type=MESH,
        )

    order = list(range(n - 1, -1, -1))
    for off in order:
        piece = peer(off)
        for step in range(1, reps):
            to = rep_peer(step)
            across(0, grad_mine.at[to, piece], grad_rep, to, my_rep, piece).start()
    store_agg.start()
    for off in order:
        piece = peer(off)
        total = grad_mine[my_rep, piece]
        for step in range(1, reps):
            to = rep_peer(step)
            across(0, grad_mine.at[to, piece], grad_rep, to, to, piece).wait_recv()
            total = total + grad_rep[to, piece]
        sum_rep[piece] = total
        if off > 0:
            send(SCATTER, sum_rep, grad_dev, off)
    receive(SCATTER, sum_rep, grad_dev)
    grad_dev[me] = sum_rep[me]
    rows_sum = grad_dev[0]
    for d in range(1, n):
        rows_sum = rows_sum + grad_dev[d]
    sum_dev[...] = rows_sum
    for off in order[:-1]:
        share(sum_dev, grad_rows, peer(off), me).start()
    for step in range(1, reps):
        across(1, sum_dev, grad_all, rep_peer(step), my_rep, me).start()
    grad_all[my_rep, me] = rows_sum
    for off in range(1, n):
        piece = peer(off)
        share(sum_dev, grad_rows, piece, piece).wait_recv()
        for step in range(1, reps):
            across(1, grad_rows.at[piece], grad_all, rep_peer(step), my_rep, piece).start()
        grad_all[my_rep, piece] = grad_rows[piece]
    for off in range(n):
        piece = peer(off)
        for step in range(1, reps):
            to = rep_peer(step)
            across(1, grad_rows.at[piece], grad_all, to, to, piece).wait_recv()
    grad_out[...] = grad_all[...]

    store_pre.wait()
    store_agg.wait()
    finish(ASK, pulls, asked)
    finish(MOVE_X, send_x, own_x)
    finish(MOVE_H, send_h, own_h)
    finish(FAR_X, send_far_x, far_x)
    finish(FAR_H, send_far_h, far_h)
    finish(PUSH_ONE, send_one, push_one)
    finish(PUSH_TWO, send_two, push_two)
    finish(SCATTER, sum_rep, grad_dev)
    for off in range(1, n):
        share(sum_dev, grad_rows, peer(off), me).wait_send()
    for off in range(n):
        piece = peer(off)
        for step in range(1, reps):
            to = rep_peer(step)
            across(0, grad_mine.at[to, piece], grad_rep, to, my_rep, piece).wait_send()
            across(1, grad_rows.at[piece], grad_all, to, my_rep, piece).wait_send()


def fused(
    features,
    history,
    new_owner,
    pull_rows,
    occupancy,
    adj_local,
    adj_boundary,
    w_first,
    bias_first,
    w_second,
    cotangent,
):
    n, reps = lax.axis_size("dev"), lax.axis_size("rep")
    height, breadth = features.shape
    cluster = height // n
    pulled = pull_rows.shape[0]
    per_peer = pulled // n
    part = breadth // (n * reps)
    vmem = pl.BlockSpec(memory_space=pltpu.VMEM)
    smem = pl.BlockSpec(memory_space=pltpu.SMEM)
    anywhere = pl.BlockSpec(memory_space=pl.ANY)
    moved = pltpu.VMEM((n, cluster, breadth), BF16)
    listed = pltpu.VMEM((n, per_peer, breadth), BF16)
    strip = pltpu.VMEM((n, part, breadth), F32)
    square = pltpu.VMEM((reps, n, part, breadth), F32)
    pre, agg, gradient = pl.pallas_call(
        functools.partial(step_kernel, n, reps),
        out_shape=(
            jax.ShapeDtypeStruct((height, breadth), BF16),
            jax.ShapeDtypeStruct((height, breadth), BF16),
            jax.ShapeDtypeStruct((reps, n, part, breadth), F32),
        ),
        in_specs=[
            vmem,
            anywhere,
            smem,
            vmem,
            smem,
            anywhere,
            anywhere,
            vmem,
            vmem,
            anywhere,
        ],
        out_specs=(anywhere, anywhere, vmem),
        scratch_shapes=[
            pltpu.VMEM((height, breadth), BF16),
            pltpu.VMEM((height, height), BF16),
            pltpu.VMEM((height, pulled), BF16),
            pltpu.VMEM((pulled, height), BF16),
            pltpu.VMEM((height, breadth), BF16),
            pltpu.VMEM((n, 1, per_peer), jnp.int32),
            pltpu.VMEM((height, pulled), BF16),
            pltpu.VMEM((pulled, height), BF16),
            moved,
            moved,
            moved,
            moved,
            listed,
            listed,
            listed,
            listed,
            listed,
            listed,
            listed,
            listed,
            pltpu.VMEM((height, breadth), F32),
            pltpu.VMEM((height, breadth), BF16),
            pltpu.VMEM((height, breadth), BF16),
            pltpu.VMEM((height, breadth), BF16),
            square,
            square,
            strip,
            strip,
            pltpu.VMEM((part, breadth), F32),
            strip,
            square,
            pltpu.SemaphoreType.DMA((4,)),
            pltpu.SemaphoreType.DMA((9, n)),
            pltpu.SemaphoreType.DMA((9, n)),
            pltpu.SemaphoreType.DMA((2, reps, n)),
            pltpu.SemaphoreType.DMA((2, reps, n)),
        ],
        compiler_params=pltpu.CompilerParams(
            collective_id=0, has_side_effects=True, vmem_limit_bytes=56 * 1024 * 1024
        ),
    )(
        features,
        history,
        new_owner,
        pull_rows.reshape(n, 1, per_peer),
        occupancy,
        adj_local,
        adj_boundary,
        w_first,
        bias_first.reshape(1, breadth),
        cotangent,
    )
    hidden = jnp.maximum(pre, jnp.zeros((), BF16))
    output = jnp.dot(agg, w_second, preferred_element_type=F32).astype(BF16)
    return hidden, output, gradient.reshape(breadth, breadth)


def fits(peers, height, pulled, breadth, everyone):
    return (
        height % (128 * peers) == 0 and pulled == 128 * peers and breadth % (8 * everyone) == 0
    )


def expand(occupied):
    return jnp.repeat(jnp.repeat(occupied, 128, axis=0), 128, axis=1).astype(jnp.bfloat16)


def dense_terms(owned, remote, adj_local, adj_boundary, occupancy):
    height = owned.shape[0]
    full_mask = expand(occupancy)
    local_tile = adj_local * full_mask[:, :height]
    edge_tile = adj_boundary * full_mask[:, height:]
    summed = jnp.dot(local_tile, owned, preferred_element_type=jnp.float32)
    summed = summed + jnp.dot(edge_tile, remote, preferred_element_type=jnp.float32)
    partial_value = lax.dot_general(
        edge_tile, owned, (((0,), (0,)), ((), ())), preferred_element_type=jnp.float32
    )
    return (summed, partial_value)


def body(
    features,
    history,
    new_owner,
    pull_rows,
    occupancy,
    adj_local,
    adj_boundary,
    w_first,
    bias_first,
    w_second,
    cotangent,
):
    peer_count = lax.axis_size("dev")
    height, breadth = features.shape
    cluster = height // peer_count
    pulled = pull_rows.shape[0]
    per_peer = pulled // peer_count
    everyone = peer_count * lax.axis_size("rep")
    if fits(peer_count, height, pulled, breadth, everyone):
        return fused(
            features,
            history,
            new_owner,
            pull_rows,
            occupancy,
            adj_local,
            adj_boundary,
            w_first,
            bias_first,
            w_second,
            cotangent,
        )
    indices = jnp.arange(peer_count, dtype=jnp.int32)
    matches = (new_owner[0][:, None] == indices[None, :]).astype(jnp.int32)
    inverse = jnp.sum(matches * indices[:, None], axis=0)

    def arrange(values):
        return values.reshape(peer_count, cluster, breadth)[inverse]

    requests = lax.all_to_all(
        pull_rows.reshape(peer_count, per_peer), "dev", split_axis=0, concat_axis=0, tiled=True
    ).reshape(pulled)

    def fetch_rows(values):
        return values[requests].reshape(peer_count, per_peer, breadth)

    selector = (requests[None, :] == jnp.arange(height, dtype=jnp.int32)[:, None]).astype(
        jnp.bfloat16
    )

    def collect(received):
        return jnp.dot(
            selector, received.reshape(pulled, breadth), preferred_element_type=jnp.float32
        )

    def layer_terms(owned, remote):
        return dense_terms(owned, remote, adj_local, adj_boundary, occupancy)

    moved_x, moved_h = (
        lax.all_to_all(arrange(features), "dev", split_axis=0, concat_axis=0, tiled=True),
        lax.all_to_all(arrange(history), "dev", split_axis=0, concat_axis=0, tiled=True),
    )
    own_x = moved_x.reshape(height, breadth)
    own_h = moved_h.reshape(height, breadth)
    far_x, far_h = (
        lax.all_to_all(fetch_rows(own_x), "dev", split_axis=0, concat_axis=0, tiled=True),
        lax.all_to_all(fetch_rows(own_h), "dev", split_axis=0, concat_axis=0, tiled=True),
    )
    summed_one, partial_one = layer_terms(own_x, far_x.reshape(pulled, breadth))
    pushed_one = lax.all_to_all(
        partial_one.astype(jnp.bfloat16).reshape(peer_count, per_peer, breadth),
        "dev",
        split_axis=0,
        concat_axis=0,
        tiled=True,
    )
    far_h = far_h.reshape(pulled, breadth)
    aggregate_one = (summed_one + collect(pushed_one)).astype(jnp.bfloat16)
    hidden = jnp.maximum(
        jnp.dot(aggregate_one, w_first, preferred_element_type=jnp.float32) + bias_first, 0.0
    ).astype(jnp.bfloat16)
    summed_two, partial_two = layer_terms(hidden, far_h)
    pushed_two = lax.all_to_all(
        partial_two.astype(jnp.bfloat16).reshape(peer_count, per_peer, breadth),
        "dev",
        split_axis=0,
        concat_axis=0,
        tiled=True,
    )
    aggregate_two = (summed_two + collect(pushed_two)).astype(jnp.bfloat16)
    output = jnp.dot(aggregate_two, w_second, preferred_element_type=jnp.float32).astype(
        jnp.bfloat16
    )
    local_grad = lax.dot_general(
        aggregate_two, cotangent, (((0,), (0,)), ((), ())), preferred_element_type=jnp.float32
    )
    slices = lax.all_to_all(
        local_grad.reshape(everyone, breadth // everyone, breadth),
        ("dev", "rep"),
        split_axis=0,
        concat_axis=0,
        tiled=True,
    )
    gradient = lax.all_gather(jnp.sum(slices, axis=0), ("dev", "rep"), axis=0, tiled=True)
    return (hidden, output, gradient)


def solution(mesh):
    return jax.shard_map(
        body,
        mesh=mesh,
        in_specs=(
            P(("dev", "rep"), None),
            P(("dev", "rep"), None),
            P(("dev", "rep"), None),
            P(("dev", "rep")),
            P(("dev", "rep"), None),
            P(("dev", "rep"), None),
            P(("dev", "rep"), None),
            P(),
            P(),
            P(),
            P(("dev", "rep"), None),
        ),
        out_specs=(P(("dev", "rep"), None), P(("dev", "rep"), None), P()),
        check_vma=False,
    )
```
